32 devices in a mesh: dp: 4 (over x, y), ep: 8 (over z, core).
Axes of the slice: x: 2, y: 2, z: 4, core: 2. Of those that a mesh axis runs over, the one named last changes fastest.
Arguments:
- x: bfloat16 [4, 8, 256, 3072], P('dp', 'ep'), parts along dimension 0
- expert: int32 [4, 8, 256, 4], P('dp', 'ep'), parts along dimension 0
- slot: int32 [4, 8, 256, 4], P('dp', 'ep'), parts along dimension 0
- gate: float32 [4, 8, 256, 4], P('dp', 'ep'), parts along dimension 0
- w_gate: bfloat16 [16, 3072, 10752], P('ep')
- w_up: bfloat16 [16, 3072, 10752], P('ep')
- w_down: bfloat16 [16, 10752, 3072], P('ep')
Outputs:
- y: bfloat16 [4, 8, 256, 3072], P('dp', 'ep'), parts along dimension 0
There are 4 independent parts. The reference program is written for one: setup_inputs(seed, part) draws one part's arguments, and reference() takes and returns one part's arrays. A program takes and returns all parts, laid end to end along the dimension named above; an argument that names none is the same for every part.
All inputs are finite; a program needn't handle non-finite values.
Results may differ from the reference program's by a relative error of at most 0.009.
Values are sent between devices in bfloat16 or wider.
A program may use at most 2 GiB of HBM per device.

```python
import jax
import jax.numpy as jnp

MEMBERS = 8
TOKENS = 256
D = 3072
FF = 10752
TOP = 4
EXPERTS = 16
SLOTS = 5 * TOKENS * TOP // (4 * EXPERTS)


def setup_inputs(seed: int = 0, part: int = 0) -> dict:
    own, k1, k2, k3, k4, k5, k6 = jax.random.split(jax.random.key(seed), 7)
    kx, ke, kl, kg = jax.random.split(jax.random.fold_in(own, part), 4)
    devices = (1, MEMBERS)
    place = jax.random.permutation(kl, jnp.arange(EXPERTS, dtype=jnp.uint32))
    slow = ((EXPERTS + (9 * place) % EXPERTS) << ((9 * place) // EXPERTS)) // EXPERTS
    wait = (jax.random.bits(ke, (*devices, TOKENS, EXPERTS), jnp.uint32) >> 10) * slow
    expert = jnp.argsort(wait, axis=-1)[..., :TOP].astype(jnp.int32)
    chosen = jax.nn.one_hot(expert, EXPERTS, dtype=jnp.int32)
    in_line = jnp.cumsum(chosen.reshape(*devices, TOKENS * TOP, EXPERTS), axis=2) - 1
    slot = jnp.sum(in_line.reshape(chosen.shape) * chosen, axis=-1)

    def one(key, rows, columns):
        return (jax.random.normal(key, (rows, columns), jnp.float32) * rows**-0.5).astype(jnp.bfloat16)

    def weights(key, rows, columns):
        return jax.lax.map(lambda k: one(k, rows, columns), jax.random.split(key, EXPERTS))

    return {
        "x": jax.random.normal(kx, (*devices, TOKENS, D), jnp.float32).astype(jnp.bfloat16),
        "expert": expert,
        "slot": slot,
        "gate": jax.nn.softmax(jax.random.normal(kg, expert.shape, jnp.float32)),
        "w_gate": weights(k1, D, FF),
        "w_up": weights(k2, D, FF),
        "w_down": weights(k3, FF, D),
    }


def einsum(form, a, b):
    return jnp.einsum(form, a.astype(jnp.float32), b.astype(jnp.float32))


def reference(x, expert, slot, gate, w_gate, w_up, w_down):
    to_expert = jax.nn.one_hot(expert, EXPERTS, dtype=jnp.bfloat16)
    to_slot = jax.nn.one_hot(slot, SLOTS, dtype=jnp.bfloat16)
    weighted = to_expert * gate[..., None].astype(jnp.bfloat16)
    dispatch = einsum("abtke,abtkc->abtec", to_expert, to_slot).astype(jnp.bfloat16)
    combine = einsum("abtke,abtkc->abtec", weighted, to_slot).astype(jnp.bfloat16)
    z = einsum("abtec,abtd->aebcd", dispatch, x).astype(jnp.bfloat16)
    h = jax.nn.silu(einsum("aebcd,edf->aebcf", z, w_gate))
    h = (h * einsum("aebcd,edf->aebcf", z, w_up)).astype(jnp.bfloat16)
    out = einsum("aebcf,efd->aebcd", h, w_down).astype(jnp.bfloat16)
    y = einsum("abtec,aebcd->abtd", combine, out)
    return y.astype(jnp.bfloat16)
```

```python
import functools

import jax
import jax.numpy as jnp
from jax import lax
from jax.experimental import pallas as pl
from jax.experimental.pallas import tpu as pltpu
from jax.sharding import PartitionSpec as P

D, FF, TOK, SLOTS, LOCAL = 3072, 10752, 256, 80, 2
ROWS = 8 * SLOTS
TILE = 512
NT = FF // TILE
EARLY = 8
HALF = 7
DT = 256
TILES = D // DT
SLOT = 6
DEEP = 5


PAIR = [(0, 1), (1, 0), (2, 3), (3, 2)]
MID = [(1, 2), (2, 1)]
OUTWARD = [(1, 0), (2, 3)]
INWARD = [(0, 1), (3, 2)]


def along(v, pairs):
    return lax.ppermute(v, "ep", [(2 * a + c, 2 * b + c) for a, b in pairs for c in range(2)])


def swap(v):
    return lax.ppermute(v, "ep", [(2 * z + c, 2 * z + 1 - c) for z in range(4) for c in range(2)])


def dot(a, b):
    return jnp.dot(a, b, preferred_element_type=jnp.float32)


def gate_up_kernel(n, *refs):
    d_ref, xs, (wg_ref, wu_ref) = refs[0], refs[1 : 1 + n], refs[1 + n : 3 + n]
    h_ref, z_ref = refs[-2:]

    @pl.when(pl.program_id(1) == 0)
    def _():
        for i in range(n):
            at = pl.ds(i * SLOTS, SLOTS)
            z_ref[at, :] = dot(d_ref[0, at, :], xs[i][...]).astype(jnp.bfloat16)

    g = dot(z_ref[...], wg_ref[0])
    u = dot(z_ref[...], wu_ref[0])
    h_ref[0] = (jax.nn.silu(g) * u).astype(jnp.bfloat16)


def gate_up(h, to_slot, xs, block, wg, wu, first, tiles):
    n = len(xs)
    rows = n * SLOTS
    once = pl.Buffered(1)
    in_specs = [pl.BlockSpec((1, rows, TOK), lambda e, j: (e, block, 0))]
    in_specs += [pl.BlockSpec((TOK, D), lambda e, j: (0, 0), pipeline_mode=once)] * n
    in_specs += [pl.BlockSpec((1, D, TILE), lambda e, j: (e, 0, first + j))] * 2
    args = [to_slot, *xs, wg, wu]
    alias = {}
    if h is not None:
        in_specs.append(pl.BlockSpec(memory_space=pl.ANY))
        alias = {len(args): 0}
        args.append(h)
    flops = 2 * LOCAL * rows * D * TILE * tiles * 2
    return pl.pallas_call(
        functools.partial(gate_up_kernel, n),
        grid=(LOCAL, tiles),
        in_specs=in_specs,
        out_specs=pl.BlockSpec((1, rows, TILE), lambda e, j: (e, block, first + j)),
        out_shape=jax.ShapeDtypeStruct((LOCAL, ROWS, FF), jnp.bfloat16),
        scratch_shapes=[pltpu.VMEM((rows, D), jnp.bfloat16)],
        input_output_aliases=alias,
        cost_estimate=pl.CostEstimate(
            flops=flops, bytes_accessed=2 * LOCAL * D * TILE * tiles * 2, transcendentals=0
        ),
        compiler_params=pltpu.CompilerParams(vmem_limit_bytes=58 * 1024 * 1024),
        name=f"gate_up_{rows}_{first}",
    )(*args)


def down_kernel(c_ref, h_hbm, w_hbm, y_ref, h_ref, w_ref, out_ref, s_ref, swap_out, fn_out, tu_out, v_out,
                swap_in, fn_in, tu_in, v_in, h_sem, w_sem, send_sem, recv_sem):
    dp, me = lax.axis_index("dp"), lax.axis_index("ep")
    z = me // 2
    mid = (z == 1) | (z == 2)
    sibling = me + 1 - 2 * (me % 2)
    partner = me + 2 - 4 * (z % 2)
    across = jnp.where(z == 1, me + 2, jnp.where(z == 2, me - 2, me))

    def h_copy(e):
        return pltpu.make_async_copy(h_hbm.at[e], h_ref.at[e], h_sem.at[e])

    def w_copy(n, e):
        columns = pl.ds(pl.multiple_of(n * DT, DT), DT)
        return pltpu.make_async_copy(w_hbm.at[e, :, columns], w_ref.at[e], w_sem.at[e])

    def send(kind, n, src, dst, to):
        return pltpu.make_async_remote_copy(
            src_ref=src.at[n % 2],
            dst_ref=dst.at[n % SLOT],
            send_sem=send_sem.at[kind, n % 2],
            recv_sem=recv_sem.at[kind, n % SLOT],
            device_id=(dp, to),
            device_id_type=pl.DeviceIdType.MESH,
        )

    swap_copy = lambda n: send(0, n, swap_out, swap_in, sibling)
    fn_copy = lambda n: send(1, n, fn_out, fn_in, partner)
    tu_copy = lambda n: send(2, n, tu_out, tu_in, across)
    v_copy = lambda n: send(3, n, v_out, v_in, partner)

    h_copy(0).start()
    w_copy(0, 0).start()
    h_copy(1).start()
    w_copy(0, 1).start()

    barrier = pltpu.get_barrier_semaphore()
    for to in (sibling, partner):
        pl.semaphore_signal(barrier, inc=1, device_id=(dp, to), device_id_type=pl.DeviceIdType.MESH)

    @pl.when(mid)
    def _():
        pl.semaphore_signal(barrier, inc=1, device_id=(dp, across), device_id_type=pl.DeviceIdType.MESH)
        pl.semaphore_wait(barrier, 3)

    @pl.when(jnp.logical_not(mid))
    def _():
        pl.semaphore_wait(barrier, 2)

    h_copy(0).wait()

    def project(n, e):
        w_copy(n, e).wait()
        out = dot(h_ref[e], w_ref[e]).astype(jnp.bfloat16)
        for b in range(8):
            out_ref[b, e * SLOTS : (e + 1) * SLOTS, :] = out[b * SLOTS : (b + 1) * SLOTS]

        @pl.when(n + 1 < TILES)
        def _():
            w_copy(n + 1, e).start()

    def step(n, _):
        @pl.when(n < TILES)
        def _():
            project(n, 0)

        @pl.when((n >= 1) & (n < TILES + 1))
        def _():
            k = n - 1
            swap_copy(k).wait_recv()
            at, got = k % DEEP, k % SLOT
            for q in range(4):
                s_ref[at, q] += swap_in[got, q].astype(jnp.float32)

            @pl.when(jnp.logical_not(mid))
            def _():
                @pl.when(k >= 2)
                def _():
                    fn_copy(k - 2).wait_send()

                fn_out[k % 2] = s_ref[at, 0:2].astype(jnp.bfloat16)
                fn_copy(k).start()

        @pl.when((n >= 2) & (n < TILES + 2) & mid)
        def _():
            k = n - 2
            at, got = k % DEEP, k % SLOT
            fn_copy(k).wait_recv()

            @pl.when(k >= 2)
            def _():
                tu_copy(k - 2).wait_send()

            tu_out[k % 2] = (s_ref[at, 0:2] + fn_in[got].astype(jnp.float32)).astype(jnp.bfloat16)
            tu_copy(k).start()

        @pl.when((n >= 3) & (n < TILES + 3))
        def _():
            k = n - 3
            at, got = k % DEEP, k % SLOT

            @pl.when(mid)
            def _():
                tu_copy(k).wait_recv()
                s_ref[at, 3] += tu_in[got, 0].astype(jnp.float32)
                s_ref[at, 2] += tu_in[got, 1].astype(jnp.float32)

            @pl.when(k >= 2)
            def _():
                v_copy(k - 2).wait_send()

            v_out[k % 2] = s_ref[at, 2].astype(jnp.bfloat16)
            v_copy(k).start()

        @pl.when(n >= 4)
        def _():
            k = n - 4
            at, got = k % DEEP, k % SLOT
            v_copy(k).wait_recv()
            columns = pl.ds(pl.multiple_of(k * DT, DT), DT)
            y_ref[:, columns] = (s_ref[at, 3] + v_in[got].astype(jnp.float32)).astype(jnp.bfloat16)

        @pl.when(n < TILES)
        def _():
            @pl.when(n == 0)
            def _():
                h_copy(1).wait()

            project(n, 1)

            @pl.when(n >= 2)
            def _():
                swap_copy(n - 2).wait_send()

            for b in range(8):
                y = dot(c_ref[b], out_ref[b])
                if b % 2:
                    swap_out[n % 2, b // 2] = y.astype(jnp.bfloat16)
                else:
                    s_ref[n % DEEP, b // 2] = y
            swap_copy(n).start()

        return 0

    lax.fori_loop(0, TILES + 4, step, 0)

    for k in (TILES - 2, TILES - 1):
        swap_copy(k).wait_send()
        v_copy(k).wait_send()

        @pl.when(mid)
        def _():
            tu_copy(k).wait_send()

        @pl.when(jnp.logical_not(mid))
        def _():
            fn_copy(k).wait_send()


def down(h, from_slot, wd):
    bf16, part = jnp.bfloat16, (TOK, DT)
    return pl.pallas_call(
        down_kernel,
        in_specs=[
            pl.BlockSpec(memory_space=pltpu.VMEM),
            pl.BlockSpec(memory_space=pl.ANY),
            pl.BlockSpec(memory_space=pl.ANY),
        ],
        out_specs=pl.BlockSpec(memory_space=pltpu.VMEM),
        out_shape=jax.ShapeDtypeStruct((TOK, D), bf16),
        scratch_shapes=[
            pltpu.VMEM((LOCAL, ROWS, FF), bf16),
            pltpu.VMEM((LOCAL, FF, DT), bf16),
            pltpu.VMEM((8, LOCAL * SLOTS, DT), bf16),
            pltpu.VMEM((DEEP, 4, *part), jnp.float32),
            pltpu.VMEM((2, 4, *part), bf16),
            pltpu.VMEM((2, 2, *part), bf16),
            pltpu.VMEM((2, 2, *part), bf16),
            pltpu.VMEM((2, *part), bf16),
            pltpu.VMEM((SLOT, 4, *part), bf16),
            pltpu.VMEM((SLOT, 2, *part), bf16),
            pltpu.VMEM((SLOT, 2, *part), bf16),
            pltpu.VMEM((SLOT, *part), bf16),
            pltpu.SemaphoreType.DMA((LOCAL,)),
            pltpu.SemaphoreType.DMA((LOCAL,)),
            pltpu.SemaphoreType.DMA((4, 2)),
            pltpu.SemaphoreType.DMA((4, SLOT)),
        ],
        cost_estimate=pl.CostEstimate(
            flops=2 * LOCAL * ROWS * FF * D, bytes_accessed=2 * LOCAL * FF * D, transcendentals=0
        ),
        compiler_params=pltpu.CompilerParams(
            vmem_limit_bytes=67_000_000, collective_id=1, has_side_effects=True
        ),
        name="down",
    )(from_slot, h, wd)


def layer(x, expert, slot, gate, wg, wu, wd):
    x, expert, slot, gate = x[0, 0], expert[0, 0], slot[0, 0], gate[0, 0]
    me = lax.axis_index("ep")
    z, core = me // 2, me % 2
    mid = (z == 1) | (z == 2)

    key = jnp.where(slot < SLOTS, expert * SLOTS + slot, -1).astype(jnp.float32)
    rounded = gate.astype(jnp.bfloat16).astype(jnp.float32)
    meta = lax.all_gather(jnp.concatenate([key, rounded], -1), "ep")
    meta, x = lax.optimization_barrier((meta, x))
    key, gates = meta[..., :4].astype(jnp.int32), meta[..., 4:]
    p = along(x, PAIR)
    m = along(x, MID)
    own_s = swap(x)
    near_z = jnp.where(z < 2, 2, 1)
    far_z = jnp.where(z < 2, 3, 0)
    order = jnp.stack([2 * a + c for a in (near_z, far_z, z ^ 1, z) for c in (core, 1 - core)])
    key, gates = key[order], gates[order]
    want = (LOCAL * me + jnp.arange(LOCAL))[:, None] * SLOTS + jnp.arange(SLOTS)
    hit = key[None, :, None] == want[:, None, :, None, None]
    to_slot = hit.any(-1).astype(jnp.bfloat16).reshape(LOCAL, ROWS, TOK)
    hit = key[:, :, None] == want.reshape(-1)[:, None]
    from_slot = jnp.sum(jnp.where(hit, gates[:, :, None], 0.0), -1).astype(jnp.bfloat16)

    h = gate_up(None, to_slot, [x, own_s], 3, wg, wu, 0, EARLY)
    p, m, h = lax.optimization_barrier((p, m, h))
    p_s = swap(p)
    n2, f2 = along(m, OUTWARD), along(p, MID)
    h = gate_up(h, to_slot, [p, p_s, x, own_s], 1, wg, wu, EARLY, HALF)
    n2, f2, h = lax.optimization_barrier((n2, f2, h))
    f3 = along(f2, OUTWARD)
    near = jnp.where(mid, m, n2)
    near_s = swap(near)
    h = gate_up(h, to_slot, [p, p_s, x, own_s], 1, wg, wu, EARLY + HALF, NT - EARLY - HALF)
    f3, h = lax.optimization_barrier((f3, h))
    far = jnp.where(mid, f2, f3)
    far_s = swap(far)
    h = gate_up(h, to_slot, [near, near_s, far, far_s, p, p_s], 0, wg, wu, 0, EARLY)
    h = gate_up(h, to_slot, [near, near_s, far, far_s], 0, wg, wu, EARLY, NT - EARLY)
    return down(h, from_slot, wd)[None, None]


def solution(mesh):
    spec = P("dp", "ep")
    return jax.shard_map(
        layer,
        mesh=mesh,
        in_specs=(spec, spec, spec, spec, P("ep"), P("ep"), P("ep")),
        out_specs=spec,
        check_vma=False,
    )
```

```python
import functools

import jax
import jax.numpy as jnp
from jax import lax
from jax.experimental import pallas as pl
from jax.experimental.pallas import tpu as pltpu
from jax.sharding import PartitionSpec as P

D, FF, TOK, SLOTS, LOCAL = 3072, 10752, 256, 80, 2
ROWS = 8 * SLOTS
TILE = 512
NT = FF // TILE
DT = 256
TILES = D // DT
SLOT = 6
DEEP = 5

EARLY, EXTRA = 9, 3
PASSES = [(0, EARLY, 480, 640), (EARLY, NT, 320, 640), (0, EXTRA, 160, 480), (EXTRA, EARLY, 0, 480), (0, EXTRA, 0, 160),
          (EARLY, NT, 0, 320)]
ITEMS = 2 * sum(p[1] - p[0] for p in PASSES)
FORWARD, LATER = 16, 34
DEPTH = 3
MESH = pl.DeviceIdType.MESH


def dot(a, b):
    return jnp.dot(a, b, preferred_element_type=jnp.float32)


def tile_of(g):
    tile, start = 0, 0
    for first, last, _, _ in PASSES:
        tile = jnp.where(g >= start, first + (g - start) // 2, tile)
        start += 2 * (last - first)
    return tile


def gate_up_kernel(x_ref, meta_ref, wg_hbm, wu_hbm, h_hbm, c_ref, x_in, meta_in, z_ref, w_ref, h_ref, w_sem, h_sem,
                   x_send, x_recv, meta_send, meta_recv):
    dp, me = lax.axis_index("dp"), lax.axis_index("ep")
    z, core = me // 2, me % 2
    mid = (z == 1) | (z == 2)
    end = jnp.logical_not(mid)
    sibling = me + 1 - 2 * core
    partner = me + 2 - 4 * (z % 2)
    across = jnp.where(z == 1, me + 2, jnp.where(z == 2, me - 2, me))
    chips = (3 - 3 * (z // 2), 2 - z // 2, z + 1 - 2 * (z % 2), z)
    sources = [2 * c + k for c in chips for k in (core, 1 - core)]

    def w_copies(g):
        columns = pl.ds(pl.multiple_of(tile_of(g) * TILE, TILE), TILE)
        at = g % DEPTH
        return [
            pltpu.make_async_copy(hbm.at[g % 2, :, columns], w_ref.at[at, i], w_sem.at[at, i])
            for i, hbm in enumerate((wg_hbm, wu_hbm))
        ]

    def x_copy(i, src, slot, to):
        return pltpu.make_async_remote_copy(
            src_ref=src,
            dst_ref=x_in.at[slot],
            send_sem=x_send.at[i],
            recv_sem=x_recv.at[slot],
            device_id=(dp, to),
            device_id_type=MESH,
        )

    to_sibling = x_copy(0, x_ref, 0, sibling)
    to_partner = x_copy(1, x_ref, 1, partner)
    to_across = x_copy(2, x_ref, 3, across)
    pass_partner = x_copy(3, x_in.at[1], 2, sibling)
    partner_across = x_copy(4, x_in.at[1], 5, across)
    near_out = x_copy(5, x_in.at[3], 3, partner)
    pass_near = x_copy(6, x_in.at[3], 4, sibling)
    far_out = x_copy(7, x_in.at[5], 5, partner)
    pass_far = x_copy(8, x_in.at[5], 6, sibling)

    def meta_copy(k):
        return pltpu.make_async_remote_copy(
            src_ref=meta_ref,
            dst_ref=meta_in.at[me],
            send_sem=meta_send.at[k],
            recv_sem=meta_recv.at[me],
            device_id=(dp, (me + k) % 8),
            device_id_type=MESH,
        )

    def meta_arrival(k):
        source = (me + k) % 8
        return pltpu.make_async_remote_copy(
            src_ref=meta_ref,
            dst_ref=meta_in.at[source],
            send_sem=meta_send.at[k],
            recv_sem=meta_recv.at[source],
            device_id=(dp, source),
            device_id_type=MESH,
        )

    for g in range(DEPTH - 1):
        for copy in w_copies(g):
            copy.start()

    barrier = pltpu.get_barrier_semaphore()
    for k in range(1, 8):
        pl.semaphore_signal(barrier, inc=1, device_id=(dp, (me + k) % 8), device_id_type=MESH)
    pl.semaphore_wait(barrier, 7)

    for k in range(1, 8):
        meta_copy(k).start()
    to_partner.start()

    @pl.when(mid)
    def _():
        to_across.start()

    to_sibling.start()
    meta_in[me] = meta_ref[...]
    for k in range(1, 8):
        meta_arrival(k).wait_recv()

    def match(b, rows):
        meta = meta_in[sources[b]]
        slot = LOCAL * SLOTS * me + lax.broadcasted_iota(jnp.int32, (rows, TOK), 0)
        slot = slot.astype(jnp.float32)
        hits = [slot == jnp.broadcast_to(meta[j : j + 1], (rows, TOK)) for j in range(4)]
        return hits, [jnp.broadcast_to(meta[4 + j : 5 + j], (rows, TOK)) for j in range(4)]

    def dispatch(b, x):
        hits, _ = match(b, LOCAL * SLOTS)
        hit = hits[0] | hits[1] | hits[2] | hits[3]
        rows = dot(jnp.where(hit, 1.0, 0.0).astype(jnp.bfloat16), x[...]).astype(jnp.bfloat16)
        for e in range(LOCAL):
            z_ref[e, b * SLOTS : (b + 1) * SLOTS, :] = rows[e * SLOTS : (e + 1) * SLOTS]

    def forward():
        to_partner.wait_recv()
        pass_partner.start()

        @pl.when(mid)
        def _():
            partner_across.start()
            to_across.wait_recv()
            near_out.start()
            pass_near.start()

    def later():
        @pl.when(mid)
        def _():
            partner_across.wait_recv()
            far_out.start()
            pass_far.start()

        @pl.when(end)
        def _():
            near_out.wait_recv()
            pass_near.start()

    def run(p, start):
        first, last, low, high = PASSES[p]
        rows, count = high - low, 2 * (last - first)

        def h_copy(g):
            columns = pl.ds(pl.multiple_of(tile_of(g) * TILE, TILE), TILE)
            return pltpu.make_async_copy(
                h_ref.at[g % 2, 0:rows], h_hbm.at[g % 2, low:high, columns], h_sem.at[g % 2]
            )

        def item(g, _):
            for copy in w_copies(g):
                copy.wait()

            @pl.when(g + DEPTH - 1 < ITEMS)
            def _():
                for copy in w_copies(g + DEPTH - 1):
                    copy.start()

            if start <= FORWARD < start + count:
                pl.when(g == FORWARD)(forward)
            if start <= LATER < start + count:
                pl.when(g == LATER)(later)

            at = g % DEPTH
            z_rows = z_ref[g % 2, low:high, :]
            gate = dot(z_rows, w_ref[at, 0])
            up = dot(z_rows, w_ref[at, 1])

            @pl.when(g >= start + 2)
            def _():
                h_copy(g - 2).wait()

            h_ref[g % 2, 0:rows, :] = (jax.nn.silu(gate) * up).astype(jnp.bfloat16)
            h_copy(g).start()
            return 0

        lax.fori_loop(start, start + count, item, 0)
        h_copy(start + count - 2).wait()
        h_copy(start + count - 1).wait()
        return start + count

    dispatch(6, x_ref)
    to_sibling.wait_recv()
    dispatch(7, x_in.at[0])
    g = run(0, 0)

    dispatch(4, x_in.at[1])
    pass_partner.wait_recv()
    dispatch(5, x_in.at[2])
    g = run(1, g)

    dispatch(2, x_in.at[3])
    pass_near.wait_recv()
    dispatch(3, x_in.at[4])
    g = run(2, g)

    @pl.when(end)
    def _():
        far_out.wait_recv()
        pass_far.start()

    for b in range(8):
        hits, gates = match(b, 256)
        weight = sum(jnp.where(hit, w, 0.0) for hit, w in zip(hits, gates))
        c_ref[b] = jnp.transpose(weight).astype(jnp.bfloat16)
    dispatch(0, x_in.at[5])
    pass_far.wait_recv()
    dispatch(1, x_in.at[6])
    g = run(3, g)
    g = run(4, g)
    run(5, g)

    for k in range(1, 8):
        meta_copy(k).wait_send()
    for copy in (to_sibling, to_partner, pass_partner, pass_near, pass_far):
        copy.wait_send()

    @pl.when(mid)
    def _():
        for copy in (to_across, partner_across, near_out, far_out):
            copy.wait_send()


def gate_up(x, meta, wg, wu):
    bf16 = jnp.bfloat16
    vmem, hbm = pl.BlockSpec(memory_space=pltpu.VMEM), pl.BlockSpec(memory_space=pl.ANY)
    return pl.pallas_call(
        gate_up_kernel,
        in_specs=[vmem, vmem, hbm, hbm],
        out_specs=[hbm, vmem],
        out_shape=[
            jax.ShapeDtypeStruct((LOCAL, ROWS, FF), bf16),
            jax.ShapeDtypeStruct((8, TOK, TOK), bf16),
        ],
        scratch_shapes=[
            pltpu.VMEM((7, TOK, D), bf16),
            pltpu.VMEM((8, 8, TOK), jnp.float32),
            pltpu.VMEM((LOCAL, ROWS, D), bf16),
            pltpu.VMEM((DEPTH, 2, D, TILE), bf16),
            pltpu.VMEM((2, 480, TILE), bf16),
            pltpu.SemaphoreType.DMA((DEPTH, 2)),
            pltpu.SemaphoreType.DMA((2,)),
            pltpu.SemaphoreType.DMA((9,)),
            pltpu.SemaphoreType.DMA((7,)),
            pltpu.SemaphoreType.DMA((8,)),
            pltpu.SemaphoreType.DMA((8,)),
        ],
        cost_estimate=pl.CostEstimate(
            flops=4 * LOCAL * ROWS * D * FF, bytes_accessed=8 * LOCAL * D * FF, transcendentals=0
        ),
        compiler_params=pltpu.CompilerParams(vmem_limit_bytes=67_000_000, collective_id=2, has_side_effects=True),
        name="gate_up",
    )(x, meta, wg, wu)


def down_kernel(c_ref, h_hbm, w_hbm, y_ref, h_ref, w_ref, out_ref, s_ref, swap_out, fn_out, tu_out, v_out,
                swap_in, fn_in, tu_in, v_in, h_sem, w_sem, send_sem, recv_sem):
    dp, me = lax.axis_index("dp"), lax.axis_index("ep")
    z = me // 2
    mid = (z == 1) | (z == 2)
    sibling = me + 1 - 2 * (me % 2)
    partner = me + 2 - 4 * (z % 2)
    across = jnp.where(z == 1, me + 2, jnp.where(z == 2, me - 2, me))

    def h_copy(e):
        return pltpu.make_async_copy(h_hbm.at[e], h_ref.at[e], h_sem.at[e])

    def w_copy(n, e):
        columns = pl.ds(pl.multiple_of(n * DT, DT), DT)
        return pltpu.make_async_copy(w_hbm.at[e, :, columns], w_ref.at[e], w_sem.at[e])

    def send(kind, n, src, dst, to):
        return pltpu.make_async_remote_copy(
            src_ref=src.at[n % 2],
            dst_ref=dst.at[n % SLOT],
            send_sem=send_sem.at[kind, n % 2],
            recv_sem=recv_sem.at[kind, n % SLOT],
            device_id=(dp, to),
            device_id_type=pl.DeviceIdType.MESH,
        )

    swap_copy = lambda n: send(0, n, swap_out, swap_in, sibling)
    fn_copy = lambda n: send(1, n, fn_out, fn_in, partner)
    tu_copy = lambda n: send(2, n, tu_out, tu_in, across)
    v_copy = lambda n: send(3, n, v_out, v_in, partner)

    h_copy(0).start()
    w_copy(0, 0).start()
    h_copy(1).start()
    w_copy(0, 1).start()

    barrier = pltpu.get_barrier_semaphore()
    for to in (sibling, partner):
        pl.semaphore_signal(barrier, inc=1, device_id=(dp, to), device_id_type=pl.DeviceIdType.MESH)

    @pl.when(mid)
    def _():
        pl.semaphore_signal(barrier, inc=1, device_id=(dp, across), device_id_type=pl.DeviceIdType.MESH)
        pl.semaphore_wait(barrier, 3)

    @pl.when(jnp.logical_not(mid))
    def _():
        pl.semaphore_wait(barrier, 2)

    h_copy(0).wait()

    def project(n, e):
        w_copy(n, e).wait()
        out = dot(h_ref[e], w_ref[e]).astype(jnp.bfloat16)
        for b in range(8):
            out_ref[b, e * SLOTS : (e + 1) * SLOTS, :] = out[b * SLOTS : (b + 1) * SLOTS]

        @pl.when(n + 1 < TILES)
        def _():
            w_copy(n + 1, e).start()

    def step(n, _):
        @pl.when(n < TILES)
        def _():
            project(n, 0)

        @pl.when((n >= 1) & (n < TILES + 1))
        def _():
            k = n - 1
            swap_copy(k).wait_recv()
            at, got = k % DEEP, k % SLOT
            for q in range(4):
                s_ref[at, q] += swap_in[got, q].astype(jnp.float32)

            @pl.when(jnp.logical_not(mid))
            def _():
                @pl.when(k >= 2)
                def _():
                    fn_copy(k - 2).wait_send()

                fn_out[k % 2] = s_ref[at, 0:2].astype(jnp.bfloat16)
                fn_copy(k).start()

        @pl.when((n >= 2) & (n < TILES + 2) & mid)
        def _():
            k = n - 2
            at, got = k % DEEP, k % SLOT
            fn_copy(k).wait_recv()

            @pl.when(k >= 2)
            def _():
                tu_copy(k - 2).wait_send()

            tu_out[k % 2] = (s_ref[at, 0:2] + fn_in[got].astype(jnp.float32)).astype(jnp.bfloat16)
            tu_copy(k).start()

        @pl.when((n >= 3) & (n < TILES + 3))
        def _():
            k = n - 3
            at, got = k % DEEP, k % SLOT

            @pl.when(mid)
            def _():
                tu_copy(k).wait_recv()
                s_ref[at, 2] += tu_in[got, 0].astype(jnp.float32)
                s_ref[at, 3] += tu_in[got, 1].astype(jnp.float32)

            @pl.when(k >= 2)
            def _():
                v_copy(k - 2).wait_send()

            v_out[k % 2] = s_ref[at, 2].astype(jnp.bfloat16)
            v_copy(k).start()

        @pl.when(n >= 4)
        def _():
            k = n - 4
            at, got = k % DEEP, k % SLOT
            v_copy(k).wait_recv()
            columns = pl.ds(pl.multiple_of(k * DT, DT), DT)
            y_ref[:, columns] = (s_ref[at, 3] + v_in[got].astype(jnp.float32)).astype(jnp.bfloat16)

        @pl.when(n < TILES)
        def _():
            @pl.when(n == 0)
            def _():
                h_copy(1).wait()

            project(n, 1)

            @pl.when(n >= 2)
            def _():
                swap_copy(n - 2).wait_send()

            for b in range(8):
                y = dot(c_ref[b, :, 0 : LOCAL * SLOTS], out_ref[b])
                if b % 2:
                    swap_out[n % 2, b // 2] = y.astype(jnp.bfloat16)
                else:
                    s_ref[n % DEEP, b // 2] = y
            swap_copy(n).start()

        return 0

    lax.fori_loop(0, TILES + 4, step, 0)

    for k in (TILES - 2, TILES - 1):
        swap_copy(k).wait_send()
        v_copy(k).wait_send()

        @pl.when(mid)
        def _():
            tu_copy(k).wait_send()

        @pl.when(jnp.logical_not(mid))
        def _():
            fn_copy(k).wait_send()


def down(h, from_slot, wd):
    bf16, part = jnp.bfloat16, (TOK, DT)
    return pl.pallas_call(
        down_kernel,
        in_specs=[
            pl.BlockSpec(memory_space=pltpu.VMEM),
            pl.BlockSpec(memory_space=pl.ANY),
            pl.BlockSpec(memory_space=pl.ANY),
        ],
        out_specs=pl.BlockSpec(memory_space=pltpu.VMEM),
        out_shape=jax.ShapeDtypeStruct((TOK, D), bf16),
        scratch_shapes=[
            pltpu.VMEM((LOCAL, ROWS, FF), bf16),
            pltpu.VMEM((LOCAL, FF, DT), bf16),
            pltpu.VMEM((8, LOCAL * SLOTS, DT), bf16),
            pltpu.VMEM((DEEP, 4, *part), jnp.float32),
            pltpu.VMEM((2, 4, *part), bf16),
            pltpu.VMEM((2, 2, *part), bf16),
            pltpu.VMEM((2, 2, *part), bf16),
            pltpu.VMEM((2, *part), bf16),
            pltpu.VMEM((SLOT, 4, *part), bf16),
            pltpu.VMEM((SLOT, 2, *part), bf16),
            pltpu.VMEM((SLOT, 2, *part), bf16),
            pltpu.VMEM((SLOT, *part), bf16),
            pltpu.SemaphoreType.DMA((LOCAL,)),
            pltpu.SemaphoreType.DMA((LOCAL,)),
            pltpu.SemaphoreType.DMA((4, 2)),
            pltpu.SemaphoreType.DMA((4, SLOT)),
        ],
        cost_estimate=pl.CostEstimate(
            flops=2 * LOCAL * ROWS * FF * D, bytes_accessed=2 * LOCAL * FF * D, transcendentals=0
        ),
        compiler_params=pltpu.CompilerParams(
            vmem_limit_bytes=67_000_000, collective_id=1, has_side_effects=True
        ),
        name="down",
    )(from_slot, h, wd)


def layer(x, expert, slot, gate, wg, wu, wd):
    x, expert, slot, gate = x[0, 0], expert[0, 0], slot[0, 0], gate[0, 0]
    key = jnp.where(slot < SLOTS, expert * SLOTS + slot, -1).astype(jnp.float32)
    rounded = gate.astype(jnp.bfloat16).astype(jnp.float32)
    meta = jnp.concatenate([key.T, rounded.T], 0)
    h, from_slot = gate_up(x, meta, wg, wu)
    return down(h, from_slot, wd)[None, None]


def solution(mesh):
    spec = P("dp", "ep")
    return jax.shard_map(
        layer,
        mesh=mesh,
        in_specs=(spec, spec, spec, spec, P("ep"), P("ep"), P("ep")),
        out_specs=spec,
        check_vma=False,
    )
```

```python
import jax
import jax.numpy as jnp
from jax import lax
from jax.experimental import pallas as pl
from jax.experimental.pallas import tpu as pltpu
from jax.sharding import PartitionSpec as P

D, FF, TOK, SLOTS, LOCAL = 3072, 10752, 256, 80, 2
ROWS = 8 * SLOTS
TILE = 512
NT = FF // TILE
DT = 256
TILES = D // DT
SLOT = 6
DEEP = 5

EARLY, EXTRA = 9, 3
PASSES = [(0, EARLY, 480, 640), (EARLY, NT, 320, 640), (0, EXTRA, 160, 480), (EXTRA, EARLY, 0, 480), (0, EXTRA, 0, 160),
          (EARLY, NT, 0, 320)]
ITEMS = 2 * sum(p[1] - p[0] for p in PASSES)
FORWARD, LATER = 16, 32
DEPTH = 5
MESH = pl.DeviceIdType.MESH


def dot(a, b):
    return jnp.dot(a, b, preferred_element_type=jnp.float32)


def tile_of(g):
    tile, start = 0, 0
    for first, last, _, _ in PASSES:
        tile = jnp.where(g >= start, first + (g - start) // 2, tile)
        start += 2 * (last - first)
    return tile


def gate_up_kernel(x_ref, meta_ref, wg_hbm, wu_hbm, h_hbm, c_ref, x_in, meta_in, z_ref, w_ref, h_ref, w_sem, h_sem,
                   x_send, x_recv, meta_send, meta_recv):
    dp, me = lax.axis_index("dp"), lax.axis_index("ep")
    z, core = me // 2, me % 2
    mid = (z == 1) | (z == 2)
    end = jnp.logical_not(mid)
    sibling = me + 1 - 2 * core
    partner = me + 2 - 4 * (z % 2)
    across = jnp.where(z == 1, me + 2, jnp.where(z == 2, me - 2, me))
    chips = (3 - 3 * (z // 2), 2 - z // 2, z + 1 - 2 * (z % 2), z)
    sources = [2 * c + k for c in chips for k in (core, 1 - core)]

    def w_copies(g):
        columns = pl.ds(pl.multiple_of(tile_of(g) * TILE, TILE), TILE)
        at = g % DEPTH
        return [
            pltpu.make_async_copy(hbm.at[g % 2, :, columns], w_ref.at[at, i], w_sem.at[at, i])
            for i, hbm in enumerate((wg_hbm, wu_hbm))
        ]

    def x_copy(i, src, slot, to):
        return pltpu.make_async_remote_copy(
            src_ref=src,
            dst_ref=x_in.at[slot],
            send_sem=x_send.at[i],
            recv_sem=x_recv.at[slot],
            device_id=(dp, to),
            device_id_type=MESH,
        )

    to_sibling = x_copy(0, x_ref, 0, sibling)
    to_partner = x_copy(1, x_ref, 1, partner)
    to_across = x_copy(2, x_ref, 3, across)
    pass_partner = x_copy(3, x_in.at[1], 2, sibling)
    partner_across = x_copy(4, x_in.at[1], 5, across)
    near_out = x_copy(5, x_in.at[3], 3, partner)
    pass_near = x_copy(6, x_in.at[3], 4, sibling)
    far_out = x_copy(7, x_in.at[5], 5, partner)
    pass_far = x_copy(8, x_in.at[5], 6, sibling)

    def meta_copy(k):
        return pltpu.make_async_remote_copy(
            src_ref=meta_ref,
            dst_ref=meta_in.at[me],
            send_sem=meta_send.at[k],
            recv_sem=meta_recv.at[me],
            device_id=(dp, (me + k) % 8),
            device_id_type=MESH,
        )

    def meta_arrival(k):
        source = (me + k) % 8
        return pltpu.make_async_remote_copy(
            src_ref=meta_ref,
            dst_ref=meta_in.at[source],
            send_sem=meta_send.at[k],
            recv_sem=meta_recv.at[source],
            device_id=(dp, source),
            device_id_type=MESH,
        )

    for g in range(DEPTH - 1):
        for copy in w_copies(g):
            copy.start()

    barrier = pltpu.get_barrier_semaphore()
    for k in range(1, 8):
        pl.semaphore_signal(barrier, inc=1, device_id=(dp, (me + k) % 8), device_id_type=MESH)
    pl.semaphore_wait(barrier, 7)

    for k in range(1, 8):
        meta_copy(k).start()
    to_partner.start()

    @pl.when(mid)
    def _():
        to_across.start()

    to_sibling.start()
    meta_in[me] = meta_ref[...]
    for k in range(1, 8):
        meta_arrival(k).wait_recv()

    def match(b, rows):
        meta = meta_in[sources[b]]
        slot = LOCAL * SLOTS * me + lax.broadcasted_iota(jnp.int32, (rows, TOK), 0)
        slot = slot.astype(jnp.float32)
        hits = [slot == jnp.broadcast_to(meta[j : j + 1], (rows, TOK)) for j in range(4)]
        return hits, [jnp.broadcast_to(meta[4 + j : 5 + j], (rows, TOK)) for j in range(4)]

    def dispatch(b, x):
        hits, _ = match(b, LOCAL * SLOTS)
        hit = hits[0] | hits[1] | hits[2] | hits[3]
        rows = dot(jnp.where(hit, 1.0, 0.0).astype(jnp.bfloat16), x[...]).astype(jnp.bfloat16)
        for e in range(LOCAL):
            z_ref[e, b * SLOTS : (b + 1) * SLOTS, :] = rows[e * SLOTS : (e + 1) * SLOTS]

    def forward():
        to_partner.wait_recv()
        pass_partner.start()

        @pl.when(mid)
        def _():
            partner_across.start()
            to_across.wait_recv()
            near_out.start()
            pass_near.start()

    def later():
        @pl.when(mid)
        def _():
            partner_across.wait_recv()
            far_out.start()
            pass_far.start()

        @pl.when(end)
        def _():
            near_out.wait_recv()
            pass_near.start()

    def run(p, start):
        first, last, low, high = PASSES[p]
        rows, count = high - low, 2 * (last - first)

        def h_copy(g):
            columns = pl.ds(pl.multiple_of(tile_of(g) * TILE, TILE), TILE)
            return pltpu.make_async_copy(
                h_ref.at[g % 2, 0:rows], h_hbm.at[g % 2, low:high, columns], h_sem.at[g % 2]
            )

        def item(g, _):
            for copy in w_copies(g):
                copy.wait()

            @pl.when(g + DEPTH - 1 < ITEMS)
            def _():
                for copy in w_copies(g + DEPTH - 1):
                    copy.start()

            if start <= FORWARD < start + count:
                pl.when(g == FORWARD)(forward)
            if start <= LATER < start + count:
                pl.when(g == LATER)(later)

            at = g % DEPTH
            z_rows = z_ref[g % 2, low:high, :]
            gate = dot(z_rows, w_ref[at, 0])
            up = dot(z_rows, w_ref[at, 1])

            @pl.when(g >= start + 2)
            def _():
                h_copy(g - 2).wait()

            h_ref[g % 2, 0:rows, :] = (jax.nn.silu(gate) * up).astype(jnp.bfloat16)
            h_copy(g).start()
            return 0

        lax.fori_loop(start, start + count, item, 0)
        h_copy(start + count - 2).wait()
        h_copy(start + count - 1).wait()
        return start + count

    dispatch(6, x_ref)
    to_sibling.wait_recv()
    dispatch(7, x_in.at[0])
    g = run(0, 0)

    dispatch(4, x_in.at[1])
    pass_partner.wait_recv()
    dispatch(5, x_in.at[2])
    g = run(1, g)

    dispatch(2, x_in.at[3])
    pass_near.wait_recv()
    dispatch(3, x_in.at[4])
    g = run(2, g)

    @pl.when(end)
    def _():
        far_out.wait_recv()
        pass_far.start()

    for b in range(8):
        hits, gates = match(b, 256)
        weight = sum(jnp.where(hit, w, 0.0) for hit, w in zip(hits, gates))
        c_ref[b] = jnp.transpose(weight).astype(jnp.bfloat16)
    dispatch(0, x_in.at[5])
    pass_far.wait_recv()
    dispatch(1, x_in.at[6])
    g = run(3, g)
    g = run(4, g)
    run(5, g)

    for k in range(1, 8):
        meta_copy(k).wait_send()
    for copy in (to_sibling, to_partner, pass_partner, pass_near, pass_far):
        copy.wait_send()

    @pl.when(mid)
    def _():
        for copy in (to_across, partner_across, near_out, far_out):
            copy.wait_send()


def gate_up(x, meta, wg, wu):
    bf16 = jnp.bfloat16
    vmem, hbm = pl.BlockSpec(memory_space=pltpu.VMEM), pl.BlockSpec(memory_space=pl.ANY)
    return pl.pallas_call(
        gate_up_kernel,
        in_specs=[vmem, vmem, hbm, hbm],
        out_specs=[hbm, vmem],
        out_shape=[
            jax.ShapeDtypeStruct((LOCAL, ROWS, FF), bf16),
            jax.ShapeDtypeStruct((8, TOK, TOK), bf16),
        ],
        scratch_shapes=[
            pltpu.VMEM((7, TOK, D), bf16),
            pltpu.VMEM((8, 8, TOK), jnp.float32),
            pltpu.VMEM((LOCAL, ROWS, D), bf16),
            pltpu.VMEM((DEPTH, 2, D, TILE), bf16),
            pltpu.VMEM((2, 480, TILE), bf16),
            pltpu.SemaphoreType.DMA((DEPTH, 2)),
            pltpu.SemaphoreType.DMA((2,)),
            pltpu.SemaphoreType.DMA((9,)),
            pltpu.SemaphoreType.DMA((7,)),
            pltpu.SemaphoreType.DMA((8,)),
            pltpu.SemaphoreType.DMA((8,)),
        ],
        cost_estimate=pl.CostEstimate(
            flops=4 * LOCAL * ROWS * D * FF, bytes_accessed=8 * LOCAL * D * FF, transcendentals=0
        ),
        compiler_params=pltpu.CompilerParams(vmem_limit_bytes=67_000_000, collective_id=2, has_side_effects=True),
        name="gate_up",
    )(x, meta, wg, wu)


def down_kernel(c_ref, h_hbm, w_hbm, y_ref, h_ref, w_ref, out_ref, s_ref, swap_out, fn_out, tu_out, v_out,
                swap_in, fn_in, tu_in, v_in, h_sem, w_sem, send_sem, recv_sem):
    dp, me = lax.axis_index("dp"), lax.axis_index("ep")
    z = me // 2
    mid = (z == 1) | (z == 2)
    sibling = me + 1 - 2 * (me % 2)
    partner = me + 2 - 4 * (z % 2)
    across = jnp.where(z == 1, me + 2, jnp.where(z == 2, me - 2, me))

    def h_copy(e):
        return pltpu.make_async_copy(h_hbm.at[e], h_ref.at[e], h_sem.at[e])

    def w_copy(n, e):
        columns = pl.ds(pl.multiple_of(n * DT, DT), DT)
        return pltpu.make_async_copy(w_hbm.at[e, :, columns], w_ref.at[e], w_sem.at[e])

    def send(kind, n, src, dst, to):
        return pltpu.make_async_remote_copy(
            src_ref=src,
            dst_ref=dst,
            send_sem=send_sem.at[kind, n % 2],
            recv_sem=recv_sem.at[kind, n % SLOT],
            device_id=(dp, to),
            device_id_type=pl.DeviceIdType.MESH,
        )

    def swap_copy(n):
        return send(0, n, swap_out.at[n % 2], swap_in.at[n % SLOT], sibling)

    def fn_copy(n, i):
        return send(1 + i, n, fn_out.at[n % 2, i], fn_in.at[n % SLOT, i], partner)

    def tu_copy(n, i):
        return send(3 + i, n, tu_out.at[n % 2, i], tu_in.at[n % SLOT, i], across)

    def v_copy(n):
        return send(5, n, v_out.at[n % 2], v_in.at[n % SLOT], partner)

    h_copy(0).start()
    w_copy(0, 0).start()

    barrier = pltpu.get_barrier_semaphore()
    for to in (sibling, partner):
        pl.semaphore_signal(barrier, inc=1, device_id=(dp, to), device_id_type=pl.DeviceIdType.MESH)

    @pl.when(mid)
    def _():
        pl.semaphore_signal(barrier, inc=1, device_id=(dp, across), device_id_type=pl.DeviceIdType.MESH)
        pl.semaphore_wait(barrier, 3)

    @pl.when(jnp.logical_not(mid))
    def _():
        pl.semaphore_wait(barrier, 2)

    h_copy(0).wait()
    h_copy(1).start()
    w_copy(0, 1).start()

    def project(n, e):
        w_copy(n, e).wait()
        out = dot(h_ref[e], w_ref[e]).astype(jnp.bfloat16)
        for b in range(8):
            out_ref[b, e * SLOTS : (e + 1) * SLOTS, :] = out[b * SLOTS : (b + 1) * SLOTS]

        @pl.when(n + 1 < TILES)
        def _():
            w_copy(n + 1, e).start()

    def step(n, _):
        @pl.when(n < TILES)
        def _():
            project(n, 0)

        @pl.when((n >= 1) & (n < TILES + 1))
        def _():
            k = n - 1
            swap_copy(k).wait_recv()
            at, got = k % DEEP, k % SLOT
            for q in range(4):
                s_ref[at, q] += swap_in[got, q].astype(jnp.float32)

            @pl.when(jnp.logical_not(mid))
            def _():
                for i in range(2):

                    @pl.when(k >= 2)
                    def _():
                        fn_copy(k - 2, i).wait_send()

                    fn_out[k % 2, i] = s_ref[at, i].astype(jnp.bfloat16)
                    fn_copy(k, i).start()

        @pl.when((n >= 2) & (n < TILES + 2) & mid)
        def _():
            k = n - 2
            at, got = k % DEEP, k % SLOT
            for i in range(2):
                fn_copy(k, i).wait_recv()

                @pl.when(k >= 2)
                def _():
                    tu_copy(k - 2, i).wait_send()

                tu_out[k % 2, i] = (s_ref[at, i] + fn_in[got, i].astype(jnp.float32)).astype(jnp.bfloat16)
                tu_copy(k, i).start()

        @pl.when((n >= 3) & (n < TILES + 3))
        def _():
            k = n - 3
            at, got = k % DEEP, k % SLOT

            @pl.when(mid)
            def _():
                tu_copy(k, 0).wait_recv()
                s_ref[at, 2] += tu_in[got, 0].astype(jnp.float32)

            @pl.when(k >= 2)
            def _():
                v_copy(k - 2).wait_send()

            v_out[k % 2] = s_ref[at, 2].astype(jnp.bfloat16)
            v_copy(k).start()

            @pl.when(mid)
            def _():
                tu_copy(k, 1).wait_recv()
                s_ref[at, 3] += tu_in[got, 1].astype(jnp.float32)

        @pl.when(n >= 4)
        def _():
            k = n - 4
            at, got = k % DEEP, k % SLOT
            v_copy(k).wait_recv()
            columns = pl.ds(pl.multiple_of(k * DT, DT), DT)
            y_ref[:, columns] = (s_ref[at, 3] + v_in[got].astype(jnp.float32)).astype(jnp.bfloat16)

        @pl.when(n < TILES)
        def _():
            @pl.when(n == 0)
            def _():
                h_copy(1).wait()

            project(n, 1)

            @pl.when(n >= 2)
            def _():
                swap_copy(n - 2).wait_send()

            for b in range(8):
                y = dot(c_ref[b, :, 0 : LOCAL * SLOTS], out_ref[b])
                if b % 2:
                    swap_out[n % 2, b // 2] = y.astype(jnp.bfloat16)
                else:
                    s_ref[n % DEEP, b // 2] = y
            swap_copy(n).start()

        return 0

    lax.fori_loop(0, TILES + 4, step, 0)

    for k in (TILES - 2, TILES - 1):
        swap_copy(k).wait_send()
        v_copy(k).wait_send()

        @pl.when(mid)
        def _():
            tu_copy(k, 0).wait_send()
            tu_copy(k, 1).wait_send()

        @pl.when(jnp.logical_not(mid))
        def _():
            fn_copy(k, 0).wait_send()
            fn_copy(k, 1).wait_send()


def down(h, from_slot, wd):
    bf16, part = jnp.bfloat16, (TOK, DT)
    return pl.pallas_call(
        down_kernel,
        in_specs=[
            pl.BlockSpec(memory_space=pltpu.VMEM),
            pl.BlockSpec(memory_space=pl.ANY),
            pl.BlockSpec(memory_space=pl.ANY),
        ],
        out_specs=pl.BlockSpec(memory_space=pltpu.VMEM),
        out_shape=jax.ShapeDtypeStruct((TOK, D), bf16),
        scratch_shapes=[
            pltpu.VMEM((LOCAL, ROWS, FF), bf16),
            pltpu.VMEM((LOCAL, FF, DT), bf16),
            pltpu.VMEM((8, LOCAL * SLOTS, DT), bf16),
            pltpu.VMEM((DEEP, 4, *part), jnp.float32),
            pltpu.VMEM((2, 4, *part), bf16),
            pltpu.VMEM((2, 2, *part), bf16),
            pltpu.VMEM((2, 2, *part), bf16),
            pltpu.VMEM((2, *part), bf16),
            pltpu.VMEM((SLOT, 4, *part), bf16),
            pltpu.VMEM((SLOT, 2, *part), bf16),
            pltpu.VMEM((SLOT, 2, *part), bf16),
            pltpu.VMEM((SLOT, *part), bf16),
            pltpu.SemaphoreType.DMA((LOCAL,)),
            pltpu.SemaphoreType.DMA((LOCAL,)),
            pltpu.SemaphoreType.DMA((6, 2)),
            pltpu.SemaphoreType.DMA((6, SLOT)),
        ],
        cost_estimate=pl.CostEstimate(
            flops=2 * LOCAL * ROWS * FF * D, bytes_accessed=2 * LOCAL * FF * D, transcendentals=0
        ),
        compiler_params=pltpu.CompilerParams(
            vmem_limit_bytes=67_000_000, collective_id=1, has_side_effects=True
        ),
        name="down",
    )(from_slot, h, wd)


def layer(x, expert, slot, gate, wg, wu, wd):
    x, expert, slot, gate = x[0, 0], expert[0, 0], slot[0, 0], gate[0, 0]
    key = jnp.where(slot < SLOTS, expert * SLOTS + slot, -1).astype(jnp.float32)
    rounded = gate.astype(jnp.bfloat16).astype(jnp.float32)
    meta = jnp.concatenate([key.T, rounded.T], 0)
    h, from_slot = gate_up(x, meta, wg, wu)
    return down(h, from_slot, wd)[None, None]


def solution(mesh):
    spec = P("dp", "ep")
    return jax.shard_map(
        layer,
        mesh=mesh,
        in_specs=(spec, spec, spec, spec, P("ep"), P("ep"), P("ep")),
        out_specs=spec,
        check_vma=False,
    )
```
